512 devices in a mesh: group: 2 (over y), row: 64 (over z, core), col: 4 (over x).
Axes of the slice: x: 4, y: 2, z: 32, core: 2. Of those that a mesh axis runs over, the one named last changes fastest.
The devices are a block of a 4x16x32 slice.
Arguments:
- compressed_absorbed_queries: bfloat16 [256, 128, 512], P(('group', 'row')), parts along dimension 0, may hold values from -6 to 6
- query_rope: bfloat16 [256, 64, 128], P(('group', 'row')), parts along dimension 0, may hold values from -6 to 6
- compressed_stored_keys: bfloat16 [256, 1024, 512], P(('group', 'row'), 'col'), parts along dimension 0, may hold values from -32 to 32
- cache_rope: bfloat16 [256, 64, 1024], P(('group', 'row'), None, 'col'), parts along dimension 0, may hold values from -32 to 32
- seq_lengths: int32 [256], P(('group', 'row')), parts along dimension 0, may hold values from 2 to 1024, as said below
- ffn_rows: bfloat16 [1024, 7168], P(('group', 'row'), 'col'), parts along dimension 0, may hold values from -6 to 6
- norm_gain: bfloat16 [7168], P('col'), may hold values from 0.099609375 to 1.8984375
- w_gate: bfloat16 [7168, 18432], P('col', 'row'), may hold values from -0.0625 to 0.0625
- w_up: bfloat16 [7168, 18432], P('col', 'row'), may hold values from -0.0625 to 0.0625
- w_down: bfloat16 [18432, 7168], P('row', 'col'), may hold values from -0.046875 to 0.046875
Outputs:
- context: bfloat16 [256, 128, 512], P(('group', 'row'), 'col'), parts along dimension 0
- ffn_out: bfloat16 [1024, 7168], P(('group', 'row'), 'col'), parts along dimension 0
The draws below stay inside these ranges and needn't reach their ends.
There are 2 independent parts, one for each index of `group`. The reference program is written for one: setup_inputs(seed, part) draws one part's arguments, and reference() takes and returns one part's arrays. A program takes and returns all parts, laid end to end along the dimension named above; an argument that names none is the same for every part. Nothing has to cross between parts.
Inputs may be any that keep to these rules, and one draw needn't show every extreme that they name: `seq_lengths`: each sequence has 2 to 1024 filled slots, the first ones of its cache, and some sequence has exactly 1024.
All inputs are finite; a program needn't handle non-finite values.
Results may differ from the reference program's by a relative error of at most 0.017.
Values may be sent and summed in bfloat16 or wider, within the bound.
No kernel may reach another device: no remote copies, remote signals or barrier semaphores. Data moves between devices by JAX's collectives and lax.ppermute only.
A program may use at most 64 MiB of HBM per device.

```python
import jax
import jax.numpy as jnp
from jax import lax

D = 7168
FF = 18432
HEADS = 128
LATENT = 512
ROPE = 64
NOPE = 128
KV_LEN = 1024
SEQS = 128
TOKENS = 512


def length_law(key):
    counts = jax.random.randint(jax.random.fold_in(key, 301), (SEQS,), 2, KV_LEN + 1)
    chosen = jax.random.randint(jax.random.fold_in(key, 302), (), 0, SEQS)
    return jnp.where(jnp.arange(SEQS) == chosen, KV_LEN, counts).astype(jnp.int32)


def question_pieces(key):
    base = jax.random.fold_in(key, 101)
    shape = (SEQS, HEADS, LATENT + ROPE)
    full = jnp.clip(jax.random.normal(base, shape, jnp.float32), -6.0, 6.0)
    return full


def key_parts(key):
    width = LATENT + ROPE
    base = jax.random.fold_in(key, 202)
    full = jnp.clip(jax.random.normal(base, (SEQS, KV_LEN, width), jnp.float32), -6.0, 6.0)
    return full


def draw_compressed_absorbed_queries(key, part):
    return question_pieces(key)[:, :, :LATENT].astype(jnp.bfloat16)


def draw_query_rope(key, part):
    return jnp.transpose(question_pieces(key)[:, :, LATENT:], (0, 2, 1)).astype(jnp.bfloat16)


def draw_compressed_stored_keys(key, part):
    return key_parts(key)[:, :, :LATENT].astype(jnp.bfloat16)


def draw_cache_rope(key, part):
    return jnp.transpose(key_parts(key)[:, :, LATENT:], (0, 2, 1)).astype(jnp.bfloat16)


def draw_seq_lengths(key, part):
    return length_law(key)


def block_scale(stream_key, extent, pieces, smallest, largest):
    gain = 1.0
    for dim, shards_of in pieces:
        heights = jax.random.uniform(jax.random.fold_in(jax.random.fold_in(stream_key, 6), dim), (shards_of,), jnp.float32, smallest / len(pieces), largest / len(pieces))
        gain = gain * jnp.repeat(jnp.exp(heights), extent[dim] // shards_of).reshape((-1,) + (1,) * (len(extent) - 1 - dim))
    return gain


def centred(key, dims, scale, reach, split=(), held_as=jnp.bfloat16):
    values = jax.random.normal(key, dims, jnp.float32) * scale
    if len(split) > 0:
        values = block_scale(key, dims, split, -0.22, 0.18) * values
    return jnp.clip(values, min=-reach, max=reach).astype(held_as)


def setup_inputs(seed: int = 0, part: int = 0) -> dict:
    seeds = jax.random.split(jax.random.key(seed), 11)
    own_keys = jax.random.split(jax.random.fold_in(seeds[10], part), 11)
    compressed_absorbed_queries = draw_compressed_absorbed_queries(jax.random.fold_in(jax.random.fold_in(seeds[10], part), 71), part)
    query_rope = draw_query_rope(jax.random.fold_in(jax.random.fold_in(seeds[10], part), 71), part)
    compressed_stored_keys = draw_compressed_stored_keys(jax.random.fold_in(jax.random.fold_in(seeds[10], part), 71), part)
    cache_rope = draw_cache_rope(jax.random.fold_in(jax.random.fold_in(seeds[10], part), 71), part)
    seq_lengths = draw_seq_lengths(jax.random.fold_in(jax.random.fold_in(seeds[10], part), 71), part)
    ffn_rows = centred(own_keys[5], (TOKENS, D), 1.0, 6.0, ((0, 64), (1, 4)))
    norm_gain = jnp.clip(1.0 + 0.18 * jax.random.normal(seeds[6], (D,), jnp.float32), 0.099609375, 1.8984375).astype(jnp.bfloat16)
    w_gate = centred(seeds[7], (D, FF), D ** -0.5, 0.0625, ((0, 4), (1, 64)))
    w_up = centred(seeds[8], (D, FF), D ** -0.5, 0.0625, ((0, 4), (1, 64)))
    w_down = centred(seeds[9], (FF, D), FF ** -0.5, 0.046875, ((0, 64), (1, 4)))
    return dict(compressed_absorbed_queries=compressed_absorbed_queries, query_rope=query_rope, compressed_stored_keys=compressed_stored_keys, cache_rope=cache_rope, seq_lengths=seq_lengths, ffn_rows=ffn_rows, norm_gain=norm_gain, w_gate=w_gate, w_up=w_up, w_down=w_down)


NEGATIVE_PADDING = -1e+30

def attend_one(packed):
    latent_query, rotary_query_part, latent_keys, rope_keys, length_one = packed
    similarity_logits = jnp.dot(latent_query, latent_keys.T, preferred_element_type=jnp.float32)
    similarity_logits = similarity_logits + jnp.dot(rotary_query_part.T, rope_keys, preferred_element_type=jnp.float32)
    similarity_logits = similarity_logits * (NOPE + ROPE) ** (-0.5)
    position = jnp.arange(KV_LEN, dtype=jnp.int32)
    visible = (position < length_one)[None, :]
    similarity_logits = jnp.where(visible, similarity_logits, NEGATIVE_PADDING)
    top_score = lax.optimization_barrier(jnp.max(similarity_logits, axis=1, keepdims=True))
    weights = jnp.where(visible, jnp.exp(similarity_logits - top_score), 0.0)
    denominator = lax.optimization_barrier(jnp.sum(weights, axis=1, keepdims=True))
    weighted = jnp.dot(weights.astype(jnp.bfloat16), latent_keys, preferred_element_type=jnp.float32)
    return (weighted / denominator).astype(jnp.bfloat16)

def reference(compressed_absorbed_queries, query_rope, compressed_stored_keys, cache_rope, seq_lengths, ffn_rows, norm_gain, w_gate, w_up, w_down):
    context = lax.map(attend_one, (compressed_absorbed_queries, query_rope, compressed_stored_keys, cache_rope, seq_lengths))
    rows_wide = ffn_rows.astype(jnp.float32)
    mean_square = lax.optimization_barrier(jnp.mean(rows_wide * rows_wide, axis=1, keepdims=True))
    normed = (rows_wide * lax.rsqrt(mean_square + 1e-06) * norm_gain.astype(jnp.float32)).astype(jnp.bfloat16)
    gate = jnp.dot(normed, w_gate, preferred_element_type=jnp.float32)
    up_proj = jnp.dot(normed, w_up, preferred_element_type=jnp.float32)
    hidden = (jax.nn.silu(gate) * up_proj).astype(jnp.bfloat16)
    ffn_out = (rows_wide + jnp.dot(hidden, w_down, preferred_element_type=jnp.float32)).astype(jnp.bfloat16)
    return (context, ffn_out)
```

```python
import jax
import jax.numpy as jnp
from jax import lax
from jax.sharding import Mesh
from jax.sharding import PartitionSpec as P

NOPE = 128
CHIP, CORE, COL = "row_0", "row_1", "col"
ROW = (CHIP, CORE)
GROUP_ROW = ("group", CHIP, CORE)
STRIDE = 4

NEGATIVE_PADDING = -1e30


def along_ring(x, hops, cores=(0, 1)):
    chips = lax.axis_size(CHIP)
    pairs = []
    for core in cores:
        step = hops if core == 0 else -hops
        pairs += [(2 * z + core, 2 * ((z + step) % chips) + core) for z in range(chips)]
    return lax.ppermute(x, ROW, pairs)


def swapped(x):
    return lax.ppermute(x, CORE, [(0, 1), (1, 0)])


def round_cols(x, hops):
    cols = lax.axis_size(COL)
    return lax.ppermute(x, COL, [(c, (c + hops) % cols) for c in range(cols)])


def exchanged(pieces, position):
    cols = lax.axis_size(COL)

    def piece(k):
        return lax.dynamic_index_in_dim(pieces, (position + k) % cols, 0, keepdims=False)

    return [piece(0)] + [round_cols(piece(k), k) for k in range(1, cols)]


def gathered_blocks(block, core):
    half = lax.axis_size(CHIP) // 2
    slots = [None] * half
    hub = block
    for start in range(0, half, STRIDE):
        last = start + STRIDE == half
        far = along_ring(hub, STRIDE, (0,) if last else (0, 1))
        for k in range(STRIDE - 1, 0, -1):
            slots[start + k - 1] = along_ring(hub, k)
        hub = far
        slots[start + STRIDE - 1] = far
    slots[-1] = jnp.where(core == 0, slots[-1], block)
    return slots


def scattered_sum(parts, core):
    half = lax.axis_size(CHIP) // 2
    carry = parts[half - 1]
    cores = (0,)
    for start in range(half - STRIDE, -1, -STRIDE):
        received = [along_ring(carry, -STRIDE, cores)]
        for k in range(STRIDE - 1, 0, -1):
            received.append(along_ring(parts[start + k - 1], -k))
        total = sum(r.astype(jnp.float32) for r in received)
        if start:
            total = total + parts[start - 1].astype(jnp.float32)
            carry = total.astype(jnp.bfloat16)
            cores = (0, 1)
    own = parts[half - 1].astype(jnp.float32)
    return total + jnp.where(core == 1, own, 0.0)


def local_partials(
    compressed_absorbed_queries,
    query_rope,
    compressed_stored_keys,
    cache_rope,
    seq_lengths,
    first_pos,
):
    logits = jnp.einsum(
        "zxm,zum->zxu",
        compressed_absorbed_queries,
        compressed_stored_keys,
        preferred_element_type=jnp.float32,
    )
    logits = logits + jnp.einsum(
        "srh,srl->shl", query_rope, cache_rope, preferred_element_type=jnp.float32
    )
    logits = logits * (NOPE + query_rope.shape[1]) ** (-0.5)
    position = first_pos + jnp.arange(compressed_stored_keys.shape[1], dtype=jnp.int32)
    visible = position[None, None, :] < seq_lengths[:, None, None]
    logits = jnp.where(visible, logits, NEGATIVE_PADDING)
    top_score = jnp.max(logits, axis=2)
    weights = jnp.where(visible, jnp.exp(logits - top_score[:, :, None]), 0.0)
    denominator = jnp.sum(weights, axis=2)
    weighted = jnp.einsum(
        "jac,jcw->jaw",
        weights.astype(jnp.bfloat16),
        compressed_stored_keys,
        preferred_element_type=jnp.float32,
    )
    return top_score, denominator, weighted


def attention(queries, query_rope, keys, cache_rope, seq_lengths, column):
    cols = lax.axis_size(COL)
    seqs, heads, latent = queries.shape
    top_score, denominator, weighted = local_partials(
        queries, query_rope, keys, cache_rope, seq_lengths, column * keys.shape[1]
    )
    by_col = weighted.astype(jnp.bfloat16).reshape(seqs, cols, heads // cols, latent)
    by_col = jnp.moveaxis(by_col, 1, 0)
    scalars = jnp.stack([top_score, denominator]).reshape(2, seqs, cols, heads // cols)
    scalars = jnp.moveaxis(scalars, 2, 0)
    values = exchanged(by_col, column)
    scalars = exchanged(scalars, column)
    tops = [s[0] for s in scalars]
    top = tops[0]
    for other in tops[1:]:
        top = jnp.maximum(top, other)
    total, context = 0.0, 0.0
    for s, v in zip(scalars, values):
        factor = jnp.exp(s[0] - top)
        total = total + s[1] * factor
        context = context + v.astype(jnp.float32) * factor[:, :, None]
    return (context / total[:, :, None]).astype(jnp.bfloat16)


def padded(x, width):
    return jnp.pad(x, ((0, 0), (0, width - x.shape[1])))


def feed_forward(ffn_rows, norm_gain, w_gate, w_up, w_down, core, column):
    cols = lax.axis_size(COL)
    rows, width = ffn_rows.shape
    units = 2 * w_gate.shape[1]
    span = -(-(units + 2) // 128) * 128
    block = jnp.concatenate([ffn_rows, swapped(ffn_rows)], axis=0)
    slots = gathered_blocks(block, core)
    gate_both = jnp.concatenate([w_gate, swapped(w_gate)], axis=1)
    up_both = jnp.concatenate([w_up, swapped(w_up)], axis=1)
    down_both = jnp.concatenate([w_down, swapped(w_down)], axis=0)
    in_weights = jnp.concatenate([padded(gate_both, span), padded(up_both, span)], axis=1)

    tokens = jnp.concatenate(slots, axis=0).astype(jnp.float32)
    squares = jnp.sum(tokens * tokens, axis=1, keepdims=True)
    coarse = lax.reduce_precision(squares, 8, 7)
    fine = squares - coarse
    scaled = (tokens * norm_gain.astype(jnp.float32)[None, :]).astype(jnp.bfloat16)
    projected = jnp.dot(scaled, in_weights, preferred_element_type=jnp.float32)
    lane = lax.broadcasted_iota(jnp.int32, (1, 2 * span), 1)
    projected = jnp.where(lane == units, coarse, projected)
    projected = jnp.where(lane == units + 1, fine, projected)
    shares = projected.astype(jnp.bfloat16).reshape(cols, -1, 2 * span)
    total = sum(s.astype(jnp.float32) for s in exchanged(shares, column))
    full = width * cols
    mean_square = (total[:, units] + total[:, units + 1]) / full
    scale = lax.rsqrt(mean_square + 1e-06)[:, None]
    gate = total[:, :units] * scale
    up = total[:, span : span + units] * scale
    hidden = (jax.nn.silu(gate) * up).astype(jnp.bfloat16)

    arrived = [hidden] + [round_cols(hidden, k) for k in range(1, cols)]
    descending = [arrived[(cols - 1 - p) % cols] for p in range(2 * cols - 1)]
    share = hidden.shape[0]
    hidden_all = lax.dynamic_slice_in_dim(
        jnp.concatenate(descending, axis=0), (cols - 1 - column) * share, cols * share, 0
    )
    partial = jnp.dot(hidden_all, down_both, preferred_element_type=jnp.float32)
    partial = partial.astype(jnp.bfloat16).reshape(len(slots), 2 * rows, width)
    total = scattered_sum([partial[d] for d in range(len(slots))], core)
    reduced = total[:rows] + swapped(total[rows:])
    return (ffn_rows.astype(jnp.float32) + reduced).astype(jnp.bfloat16)


def on_device(
    compressed_absorbed_queries,
    query_rope,
    compressed_stored_keys,
    cache_rope,
    seq_lengths,
    ffn_rows,
    norm_gain,
    w_gate,
    w_up,
    w_down,
):
    column = lax.axis_index(COL)
    core = lax.axis_index(CORE)
    ffn_out = feed_forward(ffn_rows, norm_gain, w_gate, w_up, w_down, core, column)
    context = attention(
        compressed_absorbed_queries,
        query_rope,
        compressed_stored_keys,
        cache_rope,
        seq_lengths,
        column,
    )
    return (context, ffn_out)


def solution(mesh):
    finer = Mesh(
        mesh.devices.reshape(mesh.shape["group"], mesh.shape["row"] // 2, 2, mesh.shape["col"]),
        ("group", CHIP, CORE, COL),
    )
    return jax.shard_map(
        on_device,
        mesh=finer,
        in_specs=(
            P(GROUP_ROW, None, None),
            P(GROUP_ROW, None, None),
            P(GROUP_ROW, COL, None),
            P(GROUP_ROW, None, COL),
            P(GROUP_ROW),
            P(GROUP_ROW, COL),
            P(COL),
            P(COL, ROW),
            P(COL, ROW),
            P(ROW, COL),
        ),
        out_specs=(P(GROUP_ROW, COL, None), P(GROUP_ROW, COL)),
        check_vma=False,
    )
```

```python
import jax
import jax.numpy as jnp
from jax import lax
from jax.experimental.layout import Layout, with_layout_constraint
from jax.sharding import Mesh
from jax.sharding import PartitionSpec as P

NOPE = 128
FAR, NEAR, CORE, COL = "row_far", "row_near", "row_core", "col"
CHIP = (FAR, NEAR)
ROW = (FAR, NEAR, CORE)
GROUP_ROW = ("group", *ROW)
NEAR_CHIPS = 8

NEGATIVE_PADDING = -1e30


def row_major(x):
    return with_layout_constraint(x, Layout(major_to_minor=tuple(range(x.ndim))))


def along_ring(x, hops_up, hops_down):
    chips = lax.axis_size(CHIP)
    pairs = []
    for core, hops in enumerate((hops_up, hops_down)):
        pairs += [(2 * z + core, 2 * ((z + hops) % chips) + core) for z in range(chips)]
    return lax.ppermute(x, ROW, pairs)


def swapped(x):
    return lax.ppermute(x, CORE, [(0, 1), (1, 0)])


def exchanged(pieces):
    return lax.all_to_all(pieces, COL, split_axis=0, concat_axis=0, tiled=True)


def halves_of(x, count):
    pieces = []
    for _ in range(count - 1):
        coarse = lax.reduce_precision(x, 8, 7)
        pieces.append(coarse)
        x = x - coarse
    return pieces + [x]


def with_columns(x, columns):
    lane = lax.broadcasted_iota(jnp.int32, (*(1,) * (x.ndim - 1), 128), x.ndim - 1)
    extra = jnp.zeros((*x.shape[:-1], 128), jnp.float32)
    for k, column in enumerate(columns):
        extra = jnp.where(lane == k, column[..., None], extra)
    return jnp.concatenate([x.astype(jnp.bfloat16), extra.astype(jnp.bfloat16)], axis=-1)


def local_partials(
    compressed_absorbed_queries,
    query_rope,
    compressed_stored_keys,
    cache_rope,
    seq_lengths,
    first_pos,
):
    logits = jnp.einsum(
        "zxm,zum->zxu",
        compressed_absorbed_queries,
        compressed_stored_keys,
        preferred_element_type=jnp.float32,
    )
    logits = logits + jnp.einsum(
        "srh,srl->shl", query_rope, cache_rope, preferred_element_type=jnp.float32
    )
    logits = logits * (NOPE + query_rope.shape[1]) ** (-0.5)
    position = first_pos + jnp.arange(compressed_stored_keys.shape[1], dtype=jnp.int32)
    visible = position[None, None, :] < seq_lengths[:, None, None]
    logits = jnp.where(visible, logits, NEGATIVE_PADDING)
    top_score = jnp.max(logits, axis=2)
    weights = jnp.where(visible, jnp.exp(logits - top_score[:, :, None]), 0.0)
    denominator = jnp.sum(weights, axis=2)
    weighted = jnp.einsum(
        "jac,jcw->jaw",
        weights.astype(jnp.bfloat16),
        compressed_stored_keys,
        preferred_element_type=jnp.float32,
    )
    return top_score, denominator, weighted


def attention(queries, query_rope, keys, cache_rope, seq_lengths, column):
    cols = lax.axis_size(COL)
    seqs, heads, latent = queries.shape
    top_score, denominator, weighted = local_partials(
        queries, query_rope, keys, cache_rope, seq_lengths, column * keys.shape[1]
    )
    packed = with_columns(weighted, halves_of(top_score, 3) + halves_of(denominator, 3))
    packed = jnp.moveaxis(packed.reshape(seqs, cols, heads // cols, -1), 1, 0)
    merged = exchanged(row_major(packed)).astype(jnp.float32)
    tops = merged[..., latent] + (merged[..., latent + 1] + merged[..., latent + 2])
    totals = merged[..., latent + 3] + (merged[..., latent + 4] + merged[..., latent + 5])
    factor = jnp.exp(tops - jnp.max(tops, axis=0, keepdims=True))
    total = jnp.sum(totals * factor, axis=0)
    context = jnp.sum(merged[..., :latent] * factor[..., None], axis=0)
    return (context / total[..., None]).astype(jnp.bfloat16)


def reduced_to_owner(partial):
    near = lax.axis_index(NEAR)
    size = lax.axis_size(NEAR)

    def block(hops):
        return lax.dynamic_index_in_dim(partial, (near + hops) % size, 1, keepdims=False)

    half = size // 2
    arrived = [along_ring(block(half), half, -half)]
    for hops in range(half - 1, 0, -1):
        arrived += [along_ring(block(hops), hops, hops), along_ring(block(size - hops), -hops, -hops)]
    total = block(0).astype(jnp.float32)
    for other in arrived:
        total = total + other.astype(jnp.float32)
    pieces = lax.all_to_all(row_major(total.astype(jnp.bfloat16)), FAR, 0, 0, tiled=True)
    return jnp.sum(pieces.astype(jnp.float32), axis=0)


def feed_forward(ffn_rows, norm_gain, w_gate, w_up, w_down):
    cols = lax.axis_size(COL)
    rows, width = ffn_rows.shape
    units = w_gate.shape[1]
    weights = jnp.concatenate([w_gate.T, w_up.T, w_down], axis=0)
    weights = [weights, swapped(weights)]
    gathered = lax.all_gather(ffn_rows, CHIP, axis=0, tiled=True)

    tokens = gathered.astype(jnp.float32)
    squares = jnp.sum(tokens * tokens, axis=1)
    scaled = (tokens * norm_gain.astype(jnp.float32)[None, :]).astype(jnp.bfloat16)
    projected = [
        lax.dot_general(
            scaled, w[: 2 * units], (((1,), (1,)), ((), ())), preferred_element_type=jnp.float32
        )
        for w in weights
    ]
    packed = with_columns(jnp.concatenate(projected, axis=1), halves_of(squares, 2))
    packed = row_major(packed.reshape(cols, -1, packed.shape[1]))
    total = jnp.sum(exchanged(packed).astype(jnp.float32), axis=0)
    mean_square = (total[:, 4 * units] + total[:, 4 * units + 1]) / (width * cols)
    scale = lax.rsqrt(mean_square + 1e-06)[:, None]
    total = total[:, : 4 * units] * scale
    gate = jnp.concatenate([total[:, :units], total[:, 2 * units : 3 * units]], axis=1)
    up = jnp.concatenate([total[:, units : 2 * units], total[:, 3 * units :]], axis=1)
    hidden = row_major((jax.nn.silu(gate) * up).astype(jnp.bfloat16))

    hidden = lax.all_gather(hidden, COL, axis=0, tiled=True)
    partial = sum(
        jnp.dot(
            hidden[:, k * units : (k + 1) * units],
            w[2 * units :],
            preferred_element_type=jnp.float32,
        )
        for k, w in enumerate(weights)
    )
    partial = partial.astype(jnp.bfloat16)
    partial = partial.reshape(lax.axis_size(FAR), lax.axis_size(NEAR), rows, width)
    reduced = reduced_to_owner(partial)
    return (ffn_rows.astype(jnp.float32) + reduced).astype(jnp.bfloat16)


def on_device(
    compressed_absorbed_queries,
    query_rope,
    compressed_stored_keys,
    cache_rope,
    seq_lengths,
    ffn_rows,
    norm_gain,
    w_gate,
    w_up,
    w_down,
):
    column = lax.axis_index(COL)
    ffn_out = feed_forward(ffn_rows, norm_gain, w_gate, w_up, w_down)
    context = attention(
        compressed_absorbed_queries,
        query_rope,
        compressed_stored_keys,
        cache_rope,
        seq_lengths,
        column,
    )
    return (context, ffn_out)


def solution(mesh):
    chips = mesh.shape["row"] // 2
    finer = Mesh(
        mesh.devices.reshape(
            mesh.shape["group"], chips // NEAR_CHIPS, NEAR_CHIPS, 2, mesh.shape["col"]
        ),
        ("group", *ROW, COL),
    )
    return jax.shard_map(
        on_device,
        mesh=finer,
        in_specs=(
            P(GROUP_ROW, None, None),
            P(GROUP_ROW, None, None),
            P(GROUP_ROW, COL, None),
            P(GROUP_ROW, None, COL),
            P(GROUP_ROW),
            P(GROUP_ROW, COL),
            P(COL),
            P(COL, ROW),
            P(COL, ROW),
            P(ROW, COL),
        ),
        out_specs=(P(GROUP_ROW, COL, None), P(GROUP_ROW, COL)),
        check_vma=False,
    )
```

```python
import jax
import jax.numpy as jnp
from jax import lax
from jax.experimental.layout import Layout, with_layout_constraint
from jax.sharding import Mesh
from jax.sharding import PartitionSpec as P


NOPE = 128
FAR, NEAR, CORE, COL = "row_far", "row_near", "row_core", "col"
CHIP = (FAR, NEAR)
ROW = (FAR, NEAR, CORE)
GROUP_ROW = ("group", *ROW)
NEAR_CHIPS = 8

NEGATIVE_PADDING = -1e30


def row_major(x):
    return with_layout_constraint(x, Layout(major_to_minor=tuple(range(x.ndim))))


def on_lane(chip, lane):
    return 2 * chip + (lane + chip) % 2


def along_lane(x, hops_of_first, hops_of_second):
    chips = lax.axis_size(CHIP)
    pairs = [
        (on_lane(z, lane), on_lane((z + hops) % chips, lane))
        for lane, hops in enumerate((hops_of_first, hops_of_second))
        for z in range(chips)
    ]
    return lax.ppermute(x, ROW, pairs)


def gathered_on_lane(x):
    chips = lax.axis_size(CHIP)
    lanes = [[on_lane(z, lane) for z in range(chips)] for lane in (0, 1)]
    return lax.all_gather(x, ROW, axis_index_groups=lanes, axis=0, tiled=True)


def swapped(x):
    return lax.ppermute(x, CORE, [(0, 1), (1, 0)])


def exchanged(pieces):
    return lax.all_to_all(pieces, COL, split_axis=0, concat_axis=0, tiled=True)


def halves_of(x, count):
    pieces = []
    for _ in range(count - 1):
        coarse = lax.reduce_precision(x, 8, 7)
        pieces.append(coarse)
        x = x - coarse
    return pieces + [x]


def with_columns(x, columns):
    lane = lax.broadcasted_iota(jnp.int32, (*(1,) * (x.ndim - 1), 128), x.ndim - 1)
    extra = jnp.zeros((*x.shape[:-1], 128), jnp.float32)
    for k, column in enumerate(columns):
        extra = jnp.where(lane == k, column[..., None], extra)
    return jnp.concatenate([x.astype(jnp.bfloat16), extra.astype(jnp.bfloat16)], axis=-1)


def local_partials(
    compressed_absorbed_queries,
    query_rope,
    compressed_stored_keys,
    cache_rope,
    seq_lengths,
    first_pos,
):
    logits = jnp.einsum(
        "zxm,zum->zxu",
        compressed_absorbed_queries,
        compressed_stored_keys,
        preferred_element_type=jnp.float32,
    )
    logits = logits + jnp.einsum(
        "srh,srl->shl", query_rope, cache_rope, preferred_element_type=jnp.float32
    )
    logits = logits * (NOPE + query_rope.shape[1]) ** (-0.5)
    position = first_pos + jnp.arange(compressed_stored_keys.shape[1], dtype=jnp.int32)
    visible = position[None, None, :] < seq_lengths[:, None, None]
    logits = jnp.where(visible, logits, NEGATIVE_PADDING)
    top_score = jnp.max(logits, axis=2)
    weights = jnp.where(visible, jnp.exp(logits - top_score[:, :, None]), 0.0)
    denominator = jnp.sum(weights, axis=2)
    weighted = jnp.einsum(
        "jac,jcw->jaw",
        weights.astype(jnp.bfloat16),
        compressed_stored_keys,
        preferred_element_type=jnp.float32,
    )
    return top_score, denominator, weighted


def packed_attention(queries, query_rope, keys, cache_rope, seq_lengths, column):
    cols = lax.axis_size(COL)
    seqs, heads, _ = queries.shape
    top_score, denominator, weighted = local_partials(
        queries, query_rope, keys, cache_rope, seq_lengths, column * keys.shape[1]
    )
    packed = with_columns(weighted, halves_of(top_score, 3) + halves_of(denominator, 3))
    return jnp.moveaxis(packed.reshape(seqs, cols, heads // cols, -1), 1, 0)


def merged_attention(packed, latent, column):
    cols = lax.axis_size(COL)
    merged = []
    for k in range(cols):
        piece = lax.dynamic_index_in_dim(packed, (column + k) % cols, 0, keepdims=False)
        if k:
            piece = lax.ppermute(piece, COL, [(c, (c + k) % cols) for c in range(cols)])
        merged.append(piece.astype(jnp.float32))
    tops = [m[..., latent] + (m[..., latent + 1] + m[..., latent + 2]) for m in merged]
    totals = [m[..., latent + 3] + (m[..., latent + 4] + m[..., latent + 5]) for m in merged]
    top = tops[0]
    for other in tops[1:]:
        top = jnp.maximum(top, other)
    factors = [jnp.exp(t - top) for t in tops]
    total = sum(t * f for t, f in zip(totals, factors))
    context = sum(m[..., :latent] * f[..., None] for m, f in zip(merged, factors))
    return (context / total[..., None]).astype(jnp.bfloat16)


def summed_near(partial):
    near = lax.axis_index(NEAR)
    size = lax.axis_size(NEAR)

    def block(hops):
        return lax.dynamic_index_in_dim(partial, (near + hops) % size, 1, keepdims=False)

    half = size // 2
    arrived = [along_lane(block(half), half, -half)]
    for hops in range(half - 1, 0, -1):
        arrived += [along_lane(block(hops), hops, hops), along_lane(block(size - hops), -hops, -hops)]
    total = block(0).astype(jnp.float32)
    for other in arrived:
        total = total + other.astype(jnp.float32)
    return total.astype(jnp.bfloat16)


def feed_forward(ffn_rows, norm_gain, w_gate, w_up, w_down, queries):
    cols = lax.axis_size(COL)
    rows, width = ffn_rows.shape
    units = w_gate.shape[1]
    share = units // cols
    into = [w_gate.T, w_up.T]
    into += [swapped(w) for w in into]
    gathered = gathered_on_lane(ffn_rows)

    tokens = gathered.astype(jnp.float32)
    squares = jnp.sum(tokens * tokens, axis=1)
    scaled = (tokens * norm_gain.astype(jnp.float32)[None, :]).astype(jnp.bfloat16)
    packed = [
        lax.dot_general(w, scaled, (((1,), (1,)), ((), ())), preferred_element_type=jnp.float32)
        .astype(jnp.bfloat16)
        .reshape(cols, share, -1)
        for w in into
    ]
    norms = jnp.stack(halves_of(squares, 2)).astype(jnp.bfloat16)
    norms = jnp.pad(norms, ((0, 6), (0, 0)))
    packed.append(jnp.broadcast_to(norms, (cols, *norms.shape)))
    packed = row_major(jnp.concatenate(packed, axis=1))
    packed, w_down, queries = lax.optimization_barrier((packed, w_down, queries))
    out_of = [w_down, swapped(w_down)]
    total = exchanged(packed)
    total = jnp.sum(total.astype(jnp.float32), axis=0)
    mean_square = (total[4 * share] + total[4 * share + 1]) / (width * cols)
    scale = lax.rsqrt(mean_square + 1e-06)[None, :]
    total = (total[: 4 * share] * scale).reshape(2, 2, share, -1)
    hidden = (jax.nn.silu(total[:, 0]) * total[:, 1]).astype(jnp.bfloat16)

    hidden = exchanged(row_major(jnp.broadcast_to(hidden, (cols, *hidden.shape))))
    partial = sum(
        lax.dot_general(
            hidden[:, k].reshape(units, -1),
            w,
            (((0,), (0,)), ((), ())),
            preferred_element_type=jnp.float32,
        )
        for k, w in enumerate(out_of)
    )
    partial = partial.astype(jnp.bfloat16)
    partial = partial.reshape(lax.axis_size(FAR), lax.axis_size(NEAR), rows, width)
    return partial, queries


def on_device(
    compressed_absorbed_queries,
    query_rope,
    compressed_stored_keys,
    cache_rope,
    seq_lengths,
    ffn_rows,
    norm_gain,
    w_gate,
    w_up,
    w_down,
):
    column = lax.axis_index(COL)
    partial, queries = feed_forward(
        ffn_rows, norm_gain, w_gate, w_up, w_down, compressed_absorbed_queries
    )
    packed = packed_attention(
        queries, query_rope, compressed_stored_keys, cache_rope, seq_lengths, column
    )
    near = summed_near(partial)
    pieces = lax.all_to_all(row_major(near), FAR, 0, 0, tiled=True)
    reduced = jnp.sum(pieces.astype(jnp.float32), axis=0)
    context = merged_attention(packed, queries.shape[-1], column)
    ffn_out = (ffn_rows.astype(jnp.float32) + reduced).astype(jnp.bfloat16)
    return (context, ffn_out)


def solution(mesh):
    chips = mesh.shape["row"] // 2
    finer = Mesh(
        mesh.devices.reshape(
            mesh.shape["group"], chips // NEAR_CHIPS, NEAR_CHIPS, 2, mesh.shape["col"]
        ),
        ("group", *ROW, COL),
    )
    return jax.shard_map(
        on_device,
        mesh=finer,
        in_specs=(
            P(GROUP_ROW, None, None),
            P(GROUP_ROW, None, None),
            P(GROUP_ROW, COL, None),
            P(GROUP_ROW, None, COL),
            P(GROUP_ROW),
            P(GROUP_ROW, COL),
            P(COL),
            P(COL, ROW),
            P(COL, ROW),
            P(ROW, COL),
        ),
        out_specs=(P(GROUP_ROW, COL, None), P(GROUP_ROW, COL)),
        check_vma=False,
    )
```

```python
import jax
import jax.numpy as jnp
from jax import lax
from jax.experimental import pallas as pl
from jax.experimental.pallas import tpu as pltpu
from jax.experimental.layout import Layout, with_layout_constraint
from jax.sharding import Mesh
from jax.sharding import PartitionSpec as P


NOPE = 128
FAR, NEAR, CORE, COL = "row_far", "row_near", "row_core", "col"
CHIP = (FAR, NEAR)
ROW = (FAR, NEAR, CORE)
GROUP_ROW = ("group", *ROW)
NEAR_CHIPS = 8

NEGATIVE_PADDING = -1e30


def row_major(x):
    return with_layout_constraint(x, Layout(major_to_minor=tuple(range(x.ndim))))


def on_lane(chip, lane):
    return 2 * chip + (lane + chip) % 2


def along_lane(x, hops_of_first, hops_of_second):
    chips = lax.axis_size(CHIP)
    pairs = [
        (on_lane(z, lane), on_lane((z + hops) % chips, lane))
        for lane, hops in enumerate((hops_of_first, hops_of_second))
        for z in range(chips)
    ]
    return lax.ppermute(x, ROW, pairs)


def gathered_on_lane(x):
    chips = lax.axis_size(CHIP)
    lanes = [[on_lane(z, lane) for z in range(chips)] for lane in (0, 1)]
    return lax.all_gather(x, ROW, axis_index_groups=lanes, axis=0, tiled=True)


def swapped(x):
    return lax.ppermute(x, CORE, [(0, 1), (1, 0)])


def exchanged(pieces):
    return lax.all_to_all(pieces, COL, split_axis=0, concat_axis=0, tiled=True)


def halves_of(x, count):
    pieces = []
    for _ in range(count - 1):
        coarse = lax.reduce_precision(x, 8, 7)
        pieces.append(coarse)
        x = x - coarse
    return pieces + [x]


def with_columns(x, columns):
    lane = lax.broadcasted_iota(jnp.int32, (*(1,) * (x.ndim - 1), 128), x.ndim - 1)
    extra = jnp.zeros((*x.shape[:-1], 128), jnp.float32)
    for k, column in enumerate(columns):
        extra = jnp.where(lane == k, column[..., None], extra)
    return jnp.concatenate([x.astype(jnp.bfloat16), extra.astype(jnp.bfloat16)], axis=-1)


def local_partials(
    compressed_absorbed_queries,
    query_rope,
    compressed_stored_keys,
    cache_rope,
    seq_lengths,
    first_pos,
):
    logits = jnp.einsum(
        "zxm,zum->zxu",
        compressed_absorbed_queries,
        compressed_stored_keys,
        preferred_element_type=jnp.float32,
    )
    logits = logits + jnp.einsum(
        "srh,srl->shl", query_rope, cache_rope, preferred_element_type=jnp.float32
    )
    logits = logits * (NOPE + query_rope.shape[1]) ** (-0.5)
    position = first_pos + jnp.arange(compressed_stored_keys.shape[1], dtype=jnp.int32)
    visible = position[None, None, :] < seq_lengths[:, None, None]
    logits = jnp.where(visible, logits, NEGATIVE_PADDING)
    top_score = jnp.max(logits, axis=2)
    weights = jnp.where(visible, jnp.exp(logits - top_score[:, :, None]), 0.0)
    denominator = jnp.sum(weights, axis=2)
    weighted = jnp.einsum(
        "jac,jcw->jaw",
        weights.astype(jnp.bfloat16),
        compressed_stored_keys,
        preferred_element_type=jnp.float32,
    )
    return top_score, denominator, weighted


def packed_attention(queries, query_rope, keys, cache_rope, seq_lengths, column):
    cols = lax.axis_size(COL)
    seqs, heads, _ = queries.shape
    top_score, denominator, weighted = local_partials(
        queries, query_rope, keys, cache_rope, seq_lengths, column * keys.shape[1]
    )
    packed = with_columns(weighted, halves_of(top_score, 3) + halves_of(denominator, 3))
    return jnp.moveaxis(packed.reshape(seqs, cols, heads // cols, -1), 1, 0)


def merged_attention(packed, latent, column):
    cols = lax.axis_size(COL)
    merged = []
    for k in range(cols):
        piece = lax.dynamic_index_in_dim(packed, (column + k) % cols, 0, keepdims=False)
        if k:
            piece = lax.ppermute(piece, COL, [(c, (c + k) % cols) for c in range(cols)])
        merged.append(piece.astype(jnp.float32))
    tops = [m[..., latent] + (m[..., latent + 1] + m[..., latent + 2]) for m in merged]
    totals = [m[..., latent + 3] + (m[..., latent + 4] + m[..., latent + 5]) for m in merged]
    top = tops[0]
    for other in tops[1:]:
        top = jnp.maximum(top, other)
    factors = [jnp.exp(t - top) for t in tops]
    total = sum(t * f for t, f in zip(totals, factors))
    context = sum(m[..., :latent] * f[..., None] for m, f in zip(merged, factors))
    return (context / total[..., None]).astype(jnp.bfloat16)


def summed_near(partial):
    far, size = partial.shape[:2]
    near = lax.axis_index(NEAR)
    window = size // 2
    place, side = near % window, near // window
    partial = partial.reshape(2 * far, window, *partial.shape[2:])

    def block(blocks, k):
        return lax.dynamic_index_in_dim(blocks, k, 1, keepdims=False)

    half = window // 2
    arrived = [along_lane(block(partial, (place + half) % window), half, -half)]
    for hops in range(half - 1, 0, -1):
        arrived += [
            along_lane(block(partial, (place + hops) % window), hops, hops),
            along_lane(block(partial, (place + window - hops) % window), -hops, -hops),
        ]
    total = block(partial, place).astype(jnp.float32)
    for other in arrived:
        total = total + other.astype(jnp.float32)
    total = total.astype(jnp.bfloat16).reshape(far, 2, *partial.shape[2:])
    other = along_lane(block(total, 1 - side), window, -window)
    total = block(total, side).astype(jnp.float32) + other.astype(jnp.float32)
    return total.astype(jnp.bfloat16)


def project_kernel(x_ref, gain_ref, *refs):
    *w_refs, out_ref, w_vmem, arrived = refs
    copies = [
        pltpu.make_async_copy(w_ref, w_vmem.at[k], arrived.at[k]) for k, w_ref in enumerate(w_refs)
    ]
    for copy in copies:
        copy.start()
    cols, _, _ = out_ref.shape
    share = w_vmem.shape[1] // cols
    x = x_ref[...].astype(jnp.float32)
    scaled = (x * gain_ref[...].astype(jnp.float32)).astype(jnp.bfloat16)
    squares = lax.dot_general(
        jnp.ones((8, x.shape[1]), jnp.float32),
        x * x,
        (((1,), (1,)), ((), ())),
        precision=lax.Precision.HIGHEST,
        preferred_element_type=jnp.float32,
    )
    coarse = squares.astype(jnp.bfloat16).astype(jnp.float32)
    row = lax.broadcasted_iota(jnp.int32, squares.shape, 0)
    norms = jnp.where(row == 0, coarse, squares - coarse).astype(jnp.bfloat16)
    for c in range(cols):
        out_ref[c, len(copies) * share :, :] = norms
    for k, copy in enumerate(copies):
        copy.wait()
        product = lax.dot_general(
            w_vmem[k], scaled, (((1,), (1,)), ((), ())), preferred_element_type=jnp.float32
        ).astype(jnp.bfloat16)
        for c in range(cols):
            out_ref[c, k * share : (k + 1) * share, :] = product[c * share : (c + 1) * share, :]


def projected(gathered, gain, weights, cols):
    tokens, width = gathered.shape
    units = weights[0].shape[0]
    rows = len(weights) * units // cols + 8
    whole = pl.BlockSpec(memory_space=pltpu.VMEM)
    return pl.pallas_call(
        project_kernel,
        out_shape=jax.ShapeDtypeStruct((cols, rows, tokens), jnp.bfloat16),
        in_specs=[whole, whole] + [pl.BlockSpec(memory_space=pltpu.HBM)] * len(weights),
        out_specs=whole,
        scratch_shapes=[
            pltpu.VMEM((len(weights), units, width), jnp.bfloat16),
            pltpu.SemaphoreType.DMA((len(weights),)),
        ],
        compiler_params=pltpu.CompilerParams(vmem_limit_bytes=24 << 20),
        cost_estimate=pl.CostEstimate(
            flops=2 * len(weights) * units * width * tokens,
            bytes_accessed=2 * len(weights) * units * width,
            transcendentals=0,
        ),
        name="projected",
    )(gathered, gain[None, :], *weights)


def feed_forward(ffn_rows, norm_gain, w_gate, w_up, w_down, queries):
    cols = lax.axis_size(COL)
    rows, width = ffn_rows.shape
    units = w_gate.shape[1]
    share = units // cols
    into = [w_gate.T, w_up.T]
    into += [swapped(w) for w in into]
    gathered = gathered_on_lane(ffn_rows)

    packed = projected(gathered, norm_gain, into, cols)
    packed, w_down, *queries = lax.optimization_barrier((packed, w_down, *queries))
    out_of = [w_down, swapped(w_down)]
    total = exchanged(packed)
    total = jnp.sum(total.astype(jnp.float32), axis=0)
    mean_square = (total[4 * share] + total[4 * share + 1]) / (width * cols)
    scale = lax.rsqrt(mean_square + 1e-06)[None, :]
    total = (total[: 4 * share] * scale).reshape(2, 2, share, -1)
    hidden = (jax.nn.silu(total[:, 0]) * total[:, 1]).astype(jnp.bfloat16)

    hidden = exchanged(row_major(jnp.broadcast_to(hidden, (cols, *hidden.shape))))
    partial = sum(
        lax.dot_general(
            hidden[:, k].reshape(units, -1),
            w,
            (((0,), (0,)), ((), ())),
            preferred_element_type=jnp.float32,
        )
        for k, w in enumerate(out_of)
    )
    partial = partial.astype(jnp.bfloat16)
    partial = partial.reshape(lax.axis_size(FAR), lax.axis_size(NEAR), rows, width)
    return partial, queries


def on_device(
    compressed_absorbed_queries,
    query_rope,
    compressed_stored_keys,
    cache_rope,
    seq_lengths,
    ffn_rows,
    norm_gain,
    w_gate,
    w_up,
    w_down,
):
    column = lax.axis_index(COL)
    partial, queries = feed_forward(
        ffn_rows,
        norm_gain,
        w_gate,
        w_up,
        w_down,
        (compressed_absorbed_queries, query_rope),
    )
    packed = packed_attention(
        *queries, compressed_stored_keys, cache_rope, seq_lengths, column
    )
    near = summed_near(partial)
    pieces = lax.all_to_all(row_major(near), FAR, 0, 0, tiled=True)
    reduced = jnp.sum(pieces.astype(jnp.float32), axis=0)
    context = merged_attention(packed, compressed_stored_keys.shape[-1], column)
    ffn_out = (ffn_rows.astype(jnp.float32) + reduced).astype(jnp.bfloat16)
    return (context, ffn_out)


def solution(mesh):
    chips = mesh.shape["row"] // 2
    finer = Mesh(
        mesh.devices.reshape(
            mesh.shape["group"], chips // NEAR_CHIPS, NEAR_CHIPS, 2, mesh.shape["col"]
        ),
        ("group", *ROW, COL),
    )
    return jax.shard_map(
        on_device,
        mesh=finer,
        in_specs=(
            P(GROUP_ROW, None, None),
            P(GROUP_ROW, None, None),
            P(GROUP_ROW, COL, None),
            P(GROUP_ROW, None, COL),
            P(GROUP_ROW),
            P(GROUP_ROW, COL),
            P(COL),
            P(COL, ROW),
            P(COL, ROW),
            P(ROW, COL),
        ),
        out_specs=(P(GROUP_ROW, COL, None), P(GROUP_ROW, COL)),
        check_vma=False,
    )
```

```python
import jax
import jax.numpy as jnp
from jax import lax
from jax.experimental import pallas as pl
from jax.experimental.pallas import tpu as pltpu
from jax.experimental.layout import Layout, with_layout_constraint
from jax.sharding import Mesh
from jax.sharding import PartitionSpec as P


NOPE = 128
FAR, NEAR, CORE, COL = "row_far", "row_near", "row_core", "col"
CHIP = (FAR, NEAR)
ROW = (FAR, NEAR, CORE)
GROUP_ROW = ("group", *ROW)
NEAR_CHIPS = 8

NEGATIVE_PADDING = -1e30


def row_major(x):
    return with_layout_constraint(x, Layout(major_to_minor=tuple(range(x.ndim))))


def on_lane(chip, lane):
    return 2 * chip + (lane + chip) % 2


def along_lane(x, hops_of_first, hops_of_second):
    chips = lax.axis_size(CHIP)
    pairs = [
        (on_lane(z, lane), on_lane((z + hops) % chips, lane))
        for lane, hops in enumerate((hops_of_first, hops_of_second))
        for z in range(chips)
    ]
    return lax.ppermute(x, ROW, pairs)


def gathered_on_lane(x):
    chips = lax.axis_size(CHIP)
    lanes = [[on_lane(z, lane) for z in range(chips)] for lane in (0, 1)]
    return lax.all_gather(x, ROW, axis_index_groups=lanes, axis=0, tiled=True)


def swapped(x):
    return lax.ppermute(x, CORE, [(0, 1), (1, 0)])


def exchanged(pieces):
    return lax.all_to_all(pieces, COL, split_axis=0, concat_axis=0, tiled=True)


def halves_of(x, count):
    pieces = []
    for _ in range(count - 1):
        coarse = lax.reduce_precision(x, 8, 7)
        pieces.append(coarse)
        x = x - coarse
    return pieces + [x]


def with_columns(x, columns):
    extra = jnp.stack(columns, axis=-1).astype(jnp.bfloat16)
    extra = jnp.pad(extra, [(0, 0)] * (x.ndim - 1) + [(0, 128 - len(columns))])
    return jnp.concatenate([x.astype(jnp.bfloat16), extra], axis=-1)


def local_partials(
    compressed_absorbed_queries,
    query_rope,
    compressed_stored_keys,
    cache_rope,
    seq_lengths,
    first_pos,
):
    logits = jnp.einsum(
        "zxm,zum->zxu",
        compressed_absorbed_queries,
        compressed_stored_keys,
        preferred_element_type=jnp.float32,
    )
    logits = logits + jnp.einsum(
        "srh,srl->shl", query_rope, cache_rope, preferred_element_type=jnp.float32
    )
    logits = logits * (NOPE + query_rope.shape[1]) ** (-0.5)
    position = first_pos + jnp.arange(compressed_stored_keys.shape[1], dtype=jnp.int32)
    visible = position[None, None, :] < seq_lengths[:, None, None]
    logits = jnp.where(visible, logits, NEGATIVE_PADDING)
    top_score = jnp.max(logits, axis=2)
    weights = jnp.where(visible, jnp.exp(logits - top_score[:, :, None]), 0.0)
    denominator = jnp.sum(weights, axis=2)
    weighted = jnp.einsum(
        "jac,jcw->jaw",
        weights.astype(jnp.bfloat16),
        compressed_stored_keys,
        preferred_element_type=jnp.float32,
    )
    return top_score, denominator, weighted


def packed_attention(queries, query_rope, keys, cache_rope, seq_lengths, column):
    cols = lax.axis_size(COL)
    seqs, heads, _ = queries.shape
    top_score, denominator, weighted = local_partials(
        queries, query_rope, keys, cache_rope, seq_lengths, column * keys.shape[1]
    )
    packed = with_columns(weighted, halves_of(top_score, 3) + halves_of(denominator, 3))
    return jnp.moveaxis(packed.reshape(seqs, cols, heads // cols, -1), 1, 0)


def merged_attention(packed, latent, column):
    cols = lax.axis_size(COL)
    merged = []
    for k in range(cols):
        piece = lax.dynamic_index_in_dim(packed, (column + k) % cols, 0, keepdims=False)
        if k:
            piece = lax.ppermute(piece, COL, [(c, (c + k) % cols) for c in range(cols)])
        merged.append(piece.astype(jnp.float32))
    tops = [m[..., latent] + (m[..., latent + 1] + m[..., latent + 2]) for m in merged]
    totals = [m[..., latent + 3] + (m[..., latent + 4] + m[..., latent + 5]) for m in merged]
    top = tops[0]
    for other in tops[1:]:
        top = jnp.maximum(top, other)
    factors = [jnp.exp(t - top) for t in tops]
    total = sum(t * f for t, f in zip(totals, factors))
    context = sum(m[..., :latent] * f[..., None] for m, f in zip(merged, factors))
    return (context / total[..., None]).astype(jnp.bfloat16)


def summed_near(partial):
    far, size = partial.shape[:2]
    near = lax.axis_index(NEAR)
    window = size // 2
    place, side = near % window, near // window
    partial = partial.reshape(2 * far, window, *partial.shape[2:])

    def block(blocks, k):
        return lax.dynamic_index_in_dim(blocks, k, 1, keepdims=False)

    half = window // 2
    sends = [((place + half) % window, half, -half)]
    for hops in range(half - 1, 0, -1):
        sends += [((place + hops) % window, hops, hops)]
        sends += [((place + window - hops) % window, -hops, -hops)]
    blocks = [block(partial, send[0]) for send in sends]
    arrived = [along_lane(b, *send[1:]) for b, send in zip(blocks, sends)]
    total = block(partial, place).astype(jnp.float32)
    for other in arrived:
        total = total + other.astype(jnp.float32)
    total = total.astype(jnp.bfloat16).reshape(far, 2, *partial.shape[2:])
    sent = block(total, 1 - side)
    other = along_lane(sent, window, -window)
    total = block(total, side).astype(jnp.float32) + other.astype(jnp.float32)
    return total.astype(jnp.bfloat16)


def project_kernel(x_ref, gain_ref, *refs):
    *w_refs, out_ref, w_vmem, arrived = refs
    units = w_refs[0].shape[0]
    copies = [
        pltpu.make_async_copy(w_ref, w_vmem.at[pl.ds(k * units, units)], arrived.at[k])
        for k, w_ref in enumerate(w_refs)
    ]
    for copy in copies:
        copy.start()
    cols, _, tokens = out_ref.shape
    share = units // cols
    x = x_ref[...].astype(jnp.float32)
    scaled = (x * gain_ref[...].astype(jnp.float32)).astype(jnp.bfloat16)
    squares = jnp.sum(x * x, axis=1, keepdims=True)
    squares = jnp.broadcast_to(squares, (tokens, 128)).T[:8]
    coarse = squares.astype(jnp.bfloat16).astype(jnp.float32)
    row = lax.broadcasted_iota(jnp.int32, squares.shape, 0)
    norms = jnp.where(row == 0, coarse, squares - coarse).astype(jnp.bfloat16)
    for c in range(cols):
        out_ref[c, len(copies) * share :, :] = norms
    for copy in copies:
        copy.wait()
    product = lax.dot_general(
        w_vmem[...], scaled, (((1,), (1,)), ((), ())), preferred_element_type=jnp.float32
    ).astype(jnp.bfloat16)
    for k in range(len(copies)):
        for c in range(cols):
            start = k * units + c * share
            out_ref[c, k * share : (k + 1) * share, :] = product[start : start + share, :]


def projected(gathered, gain, weights, cols):
    tokens, width = gathered.shape
    units = weights[0].shape[0]
    rows = len(weights) * units // cols + 8
    whole = pl.BlockSpec(memory_space=pltpu.VMEM)
    return pl.pallas_call(
        project_kernel,
        out_shape=jax.ShapeDtypeStruct((cols, rows, tokens), jnp.bfloat16),
        in_specs=[whole, whole] + [pl.BlockSpec(memory_space=pltpu.HBM)] * len(weights),
        out_specs=whole,
        scratch_shapes=[
            pltpu.VMEM((len(weights) * units, width), jnp.bfloat16),
            pltpu.SemaphoreType.DMA((len(weights),)),
        ],
        compiler_params=pltpu.CompilerParams(vmem_limit_bytes=24 << 20),
        cost_estimate=pl.CostEstimate(
            flops=2 * len(weights) * units * width * tokens,
            bytes_accessed=2 * len(weights) * units * width,
            transcendentals=0,
        ),
        name="projected",
    )(gathered, gain, *weights)


def feed_forward(ffn_rows, norm_gain, w_gate, w_up, w_down, queries):
    cols = lax.axis_size(COL)
    rows, width = ffn_rows.shape
    units = w_gate.shape[1]
    share = units // cols
    into = [w_gate.T, w_up.T]
    into += [swapped(w) for w in into]
    gathered = gathered_on_lane(ffn_rows)

    packed = projected(gathered, norm_gain, into, cols)
    packed, w_down, *queries = lax.optimization_barrier((packed, w_down, *queries))
    out_of = [w_down, swapped(w_down)]
    total = exchanged(packed)
    total = jnp.sum(total.astype(jnp.float32), axis=0)
    mean_square = (total[4 * share] + total[4 * share + 1]) / (width * cols)
    scale = lax.rsqrt(mean_square + 1e-06)[None, :]
    total = (total[: 4 * share] * scale).reshape(2, 2, share, -1)
    hidden = (jax.nn.silu(total[:, 0]) * total[:, 1]).astype(jnp.bfloat16)

    hidden = exchanged(row_major(jnp.broadcast_to(hidden, (cols, *hidden.shape))))
    partial = sum(
        lax.dot_general(
            hidden[:, k].reshape(units, -1),
            w,
            (((0,), (0,)), ((), ())),
            preferred_element_type=jnp.float32,
        )
        for k, w in enumerate(out_of)
    )
    partial = partial.astype(jnp.bfloat16)
    partial = partial.reshape(lax.axis_size(FAR), lax.axis_size(NEAR), rows, width)
    return partial, queries


def on_device(
    compressed_absorbed_queries,
    query_rope,
    compressed_stored_keys,
    cache_rope,
    seq_lengths,
    ffn_rows,
    norm_gain,
    w_gate,
    w_up,
    w_down,
):
    column = lax.axis_index(COL)
    partial, queries = feed_forward(
        ffn_rows,
        norm_gain,
        w_gate,
        w_up,
        w_down,
        (compressed_absorbed_queries, query_rope, cache_rope, seq_lengths, column),
    )
    queries, query_rope, cache_rope, seq_lengths, position = queries
    packed = packed_attention(
        queries, query_rope, compressed_stored_keys, cache_rope, seq_lengths, position
    )
    near = summed_near(partial)
    pieces = lax.all_to_all(row_major(near), FAR, 0, 0, tiled=True)
    reduced = jnp.sum(pieces.astype(jnp.float32), axis=0)
    context = merged_attention(packed, compressed_stored_keys.shape[-1], column)
    ffn_out = (ffn_rows.astype(jnp.float32) + reduced).astype(jnp.bfloat16)
    return (context, ffn_out)


def solution(mesh):
    chips = mesh.shape["row"] // 2
    finer = Mesh(
        mesh.devices.reshape(
            mesh.shape["group"], chips // NEAR_CHIPS, NEAR_CHIPS, 2, mesh.shape["col"]
        ),
        ("group", *ROW, COL),
    )
    return jax.shard_map(
        on_device,
        mesh=finer,
        in_specs=(
            P(GROUP_ROW, None, None),
            P(GROUP_ROW, None, None),
            P(GROUP_ROW, COL, None),
            P(GROUP_ROW, None, COL),
            P(GROUP_ROW),
            P(GROUP_ROW, COL),
            P(COL),
            P(COL, ROW),
            P(COL, ROW),
            P(ROW, COL),
        ),
        out_specs=(P(GROUP_ROW, COL, None), P(GROUP_ROW, COL)),
        check_vma=False,
    )
```

```python
import jax
import jax.numpy as jnp
from jax import lax
from jax.experimental import pallas as pl
from jax.experimental.pallas import tpu as pltpu
from jax.experimental.layout import Layout, with_layout_constraint
from jax.sharding import Mesh
from jax.sharding import PartitionSpec as P


NOPE = 128
FAR, NEAR, CORE, COL = "row_far", "row_near", "row_core", "col"
CHIP = (FAR, NEAR)
ROW = (FAR, NEAR, CORE)
GROUP_ROW = ("group", *ROW)
NEAR_CHIPS = 8

NEGATIVE_PADDING = -1e30


def row_major(x):
    return with_layout_constraint(x, Layout(major_to_minor=tuple(range(x.ndim))))


def on_lane(chip, lane):
    return 2 * chip + (lane + chip) % 2


def along_lane(x, hops_of_first, hops_of_second):
    chips = lax.axis_size(CHIP)
    pairs = [
        (on_lane(z, lane), on_lane((z + hops) % chips, lane))
        for lane, hops in enumerate((hops_of_first, hops_of_second))
        for z in range(chips)
    ]
    return lax.ppermute(x, ROW, pairs)


def gathered_on_lane(x):
    chips = lax.axis_size(CHIP)
    lanes = [[on_lane(z, lane) for z in range(chips)] for lane in (0, 1)]
    return lax.all_gather(x, ROW, axis_index_groups=lanes, axis=0, tiled=True)


def swapped(x):
    return lax.ppermute(x, CORE, [(0, 1), (1, 0)])


def exchanged(pieces):
    return lax.all_to_all(pieces, COL, split_axis=0, concat_axis=0, tiled=True)


def halves_of(x, count):
    pieces = []
    for _ in range(count - 1):
        coarse = lax.reduce_precision(x, 8, 7)
        pieces.append(coarse)
        x = x - coarse
    return pieces + [x]


def with_columns(x, columns):
    extra = jnp.stack(columns, axis=-1).astype(jnp.bfloat16)
    extra = jnp.pad(extra, [(0, 0)] * (x.ndim - 1) + [(0, 128 - len(columns))])
    return jnp.concatenate([x.astype(jnp.bfloat16), extra], axis=-1)


def local_partials(
    compressed_absorbed_queries,
    query_rope,
    compressed_stored_keys,
    cache_rope,
    seq_lengths,
    first_pos,
):
    logits = jnp.einsum(
        "zxm,zum->zxu",
        compressed_absorbed_queries,
        compressed_stored_keys,
        preferred_element_type=jnp.float32,
    )
    logits = logits + jnp.einsum(
        "srh,srl->shl", query_rope, cache_rope, preferred_element_type=jnp.float32
    )
    logits = logits * (NOPE + query_rope.shape[1]) ** (-0.5)
    position = first_pos + jnp.arange(compressed_stored_keys.shape[1], dtype=jnp.int32)
    visible = position[None, None, :] < seq_lengths[:, None, None]
    logits = jnp.where(visible, logits, NEGATIVE_PADDING)
    top_score = jnp.max(logits, axis=2)
    weights = jnp.where(visible, jnp.exp(logits - top_score[:, :, None]), 0.0)
    denominator = jnp.sum(weights, axis=2)
    weighted = jnp.einsum(
        "jac,jcw->jaw",
        weights.astype(jnp.bfloat16),
        compressed_stored_keys,
        preferred_element_type=jnp.float32,
    )
    return top_score, denominator, weighted


def packed_attention(queries, query_rope, keys, cache_rope, seq_lengths, column):
    cols = lax.axis_size(COL)
    seqs, heads, _ = queries.shape
    top_score, denominator, weighted = local_partials(
        queries, query_rope, keys, cache_rope, seq_lengths, column * keys.shape[1]
    )
    packed = with_columns(weighted, halves_of(top_score, 3) + halves_of(denominator, 3))
    return jnp.moveaxis(packed.reshape(seqs, cols, heads // cols, -1), 1, 0)


def merged_attention(packed, latent):
    merged = exchanged(row_major(packed))
    merged = merged.astype(jnp.float32)
    tops = merged[..., latent] + (merged[..., latent + 1] + merged[..., latent + 2])
    totals = merged[..., latent + 3] + (merged[..., latent + 4] + merged[..., latent + 5])
    factor = jnp.exp(tops - jnp.max(tops, axis=0, keepdims=True))
    total = jnp.sum(totals * factor, axis=0)
    context = jnp.sum(merged[..., :latent] * factor[..., None], axis=0)
    return (context / total[..., None]).astype(jnp.bfloat16)


def summed_near(partial):
    far, size = partial.shape[:2]
    near = lax.axis_index(NEAR)
    window = size // 2
    place, side = near % window, near // window
    partial = partial.reshape(2 * far, window, *partial.shape[2:])

    def block(blocks, k):
        return lax.dynamic_index_in_dim(blocks, k, 1, keepdims=False)

    half = window // 2
    sends = [((place + half) % window, half, -half)]
    for hops in range(half - 1, 0, -1):
        sends += [((place + hops) % window, hops, hops)]
        sends += [((place + window - hops) % window, -hops, -hops)]
    blocks = [block(partial, send[0]) for send in sends]
    arrived = [along_lane(b, *send[1:]) for b, send in zip(blocks, sends)]
    total = block(partial, place).astype(jnp.float32)
    for other in arrived:
        total = total + other.astype(jnp.float32)
    total = total.astype(jnp.bfloat16).reshape(far, 2, *partial.shape[2:])
    sent = block(total, 1 - side)
    other = along_lane(sent, window, -window)
    total = block(total, side).astype(jnp.float32) + other.astype(jnp.float32)
    return total.astype(jnp.bfloat16)


def project_kernel(x_ref, gain_ref, *refs):
    *w_refs, out_ref, w_vmem, arrived = refs
    units = w_refs[0].shape[0]
    copies = [
        pltpu.make_async_copy(w_ref, w_vmem.at[pl.ds(k * units, units)], arrived.at[k])
        for k, w_ref in enumerate(w_refs)
    ]
    for copy in copies:
        copy.start()
    cols, _, tokens = out_ref.shape
    share = units // cols
    x = x_ref[...].astype(jnp.float32)
    scaled = (x * gain_ref[...].astype(jnp.float32)).astype(jnp.bfloat16)
    squares = jnp.sum(x * x, axis=1, keepdims=True)
    squares = jnp.broadcast_to(squares, (tokens, 128)).T[:8]
    coarse = squares.astype(jnp.bfloat16).astype(jnp.float32)
    row = lax.broadcasted_iota(jnp.int32, squares.shape, 0)
    norms = jnp.where(row == 0, coarse, squares - coarse).astype(jnp.bfloat16)
    for c in range(cols):
        out_ref[c, len(copies) * share :, :] = norms
    for copy in copies:
        copy.wait()
    product = lax.dot_general(
        w_vmem[...], scaled, (((1,), (1,)), ((), ())), preferred_element_type=jnp.float32
    ).astype(jnp.bfloat16)
    for k in range(len(copies)):
        for c in range(cols):
            start = k * units + c * share
            out_ref[c, k * share : (k + 1) * share, :] = product[start : start + share, :]


def projected(gathered, gain, weights, cols):
    tokens, width = gathered.shape
    units = weights[0].shape[0]
    rows = len(weights) * units // cols + 8
    whole = pl.BlockSpec(memory_space=pltpu.VMEM)
    return pl.pallas_call(
        project_kernel,
        out_shape=jax.ShapeDtypeStruct((cols, rows, tokens), jnp.bfloat16),
        in_specs=[whole, whole] + [pl.BlockSpec(memory_space=pltpu.HBM)] * len(weights),
        out_specs=whole,
        scratch_shapes=[
            pltpu.VMEM((len(weights) * units, width), jnp.bfloat16),
            pltpu.SemaphoreType.DMA((len(weights),)),
        ],
        compiler_params=pltpu.CompilerParams(vmem_limit_bytes=24 << 20),
        cost_estimate=pl.CostEstimate(
            flops=2 * len(weights) * units * width * tokens,
            bytes_accessed=2 * len(weights) * units * width,
            transcendentals=0,
        ),
        name="projected",
    )(gathered, gain, *weights)


def feed_forward(ffn_rows, norm_gain, w_gate, w_up, w_down, queries):
    cols = lax.axis_size(COL)
    rows, width = ffn_rows.shape
    units = w_gate.shape[1]
    share = units // cols
    into = [w_gate.T, w_up.T]
    into += [swapped(w) for w in into]
    gathered = gathered_on_lane(ffn_rows)

    packed = projected(gathered, norm_gain, into, cols)
    packed, w_down, *queries = lax.optimization_barrier((packed, w_down, *queries))
    out_of = [w_down, swapped(w_down)]
    total = exchanged(packed)
    total = jnp.sum(total.astype(jnp.float32), axis=0)
    mean_square = (total[4 * share] + total[4 * share + 1]) / (width * cols)
    scale = lax.rsqrt(mean_square + 1e-06)[None, :]
    total = (total[: 4 * share] * scale).reshape(2, 2, share, -1)
    hidden = (jax.nn.silu(total[:, 0]) * total[:, 1]).astype(jnp.bfloat16)

    hidden = row_major(jnp.broadcast_to(hidden, (cols, *hidden.shape)))
    hidden = exchanged(hidden)
    partial = sum(
        lax.dot_general(
            hidden[:, k].reshape(units, -1),
            w,
            (((0,), (0,)), ((), ())),
            preferred_element_type=jnp.float32,
        )
        for k, w in enumerate(out_of)
    )
    partial = partial.astype(jnp.bfloat16)
    partial = partial.reshape(lax.axis_size(FAR), lax.axis_size(NEAR), rows, width)
    return partial, queries


def on_device(
    compressed_absorbed_queries,
    query_rope,
    compressed_stored_keys,
    cache_rope,
    seq_lengths,
    ffn_rows,
    norm_gain,
    w_gate,
    w_up,
    w_down,
):
    column = lax.axis_index(COL)
    partial, queries = feed_forward(
        ffn_rows,
        norm_gain,
        w_gate,
        w_up,
        w_down,
        (compressed_absorbed_queries, query_rope, cache_rope, seq_lengths, column),
    )
    queries, query_rope, cache_rope, seq_lengths, position = queries
    packed = packed_attention(
        queries, query_rope, compressed_stored_keys, cache_rope, seq_lengths, position
    )
    near = summed_near(partial)
    pieces = lax.all_to_all(row_major(near), FAR, 0, 0, tiled=True)
    reduced = jnp.sum(pieces.astype(jnp.float32), axis=0)
    context = merged_attention(packed, compressed_stored_keys.shape[-1])
    ffn_out = (ffn_rows.astype(jnp.float32) + reduced).astype(jnp.bfloat16)
    return (context, ffn_out)


def solution(mesh):
    chips = mesh.shape["row"] // 2
    finer = Mesh(
        mesh.devices.reshape(
            mesh.shape["group"], chips // NEAR_CHIPS, NEAR_CHIPS, 2, mesh.shape["col"]
        ),
        ("group", *ROW, COL),
    )
    return jax.shard_map(
        on_device,
        mesh=finer,
        in_specs=(
            P(GROUP_ROW, None, None),
            P(GROUP_ROW, None, None),
            P(GROUP_ROW, COL, None),
            P(GROUP_ROW, None, COL),
            P(GROUP_ROW),
            P(GROUP_ROW, COL),
            P(COL),
            P(COL, ROW),
            P(COL, ROW),
            P(ROW, COL),
        ),
        out_specs=(P(GROUP_ROW, COL, None), P(GROUP_ROW, COL)),
        check_vma=False,
    )
```

```python
import jax
import jax.numpy as jnp
from jax import lax
from jax.experimental import pallas as pl
from jax.experimental.pallas import tpu as pltpu
from jax.experimental.layout import Layout, with_layout_constraint
from jax.sharding import Mesh
from jax.sharding import PartitionSpec as P


NOPE = 128
FAR, NEAR, CORE, COL = "row_far", "row_near", "row_core", "col"
CHIP = (FAR, NEAR)
ROW = (FAR, NEAR, CORE)
GROUP_ROW = ("group", *ROW)
NEAR_CHIPS = 8

NEGATIVE_PADDING = -1e30


def row_major(x):
    return with_layout_constraint(x, Layout(major_to_minor=tuple(range(x.ndim))))


def on_lane(chip, lane):
    return 2 * chip + (lane + chip) % 2


def along_lane(x, hops_of_first, hops_of_second):
    chips = lax.axis_size(CHIP)
    pairs = [
        (on_lane(z, lane), on_lane((z + hops) % chips, lane))
        for lane, hops in enumerate((hops_of_first, hops_of_second))
        for z in range(chips)
    ]
    return lax.ppermute(x, ROW, pairs)


def gathered_on_lane(x):
    chips = lax.axis_size(CHIP)
    lanes = [[on_lane(z, lane) for z in range(chips)] for lane in (0, 1)]
    return lax.all_gather(x, ROW, axis_index_groups=lanes, axis=0, tiled=True)


def swapped(x):
    return lax.ppermute(x, CORE, [(0, 1), (1, 0)])


def exchanged(pieces):
    return lax.all_to_all(pieces, COL, split_axis=0, concat_axis=0, tiled=True)


def halves_of(x, count):
    pieces = []
    for _ in range(count - 1):
        coarse = lax.reduce_precision(x, 8, 7)
        pieces.append(coarse)
        x = x - coarse
    return pieces + [x]


def with_columns(x, columns):
    extra = jnp.stack(columns, axis=-1).astype(jnp.bfloat16)
    extra = jnp.pad(extra, [(0, 0)] * (x.ndim - 1) + [(0, 128 - len(columns))])
    return jnp.concatenate([x.astype(jnp.bfloat16), extra], axis=-1)


def local_partials(
    compressed_absorbed_queries,
    query_rope,
    compressed_stored_keys,
    cache_rope,
    seq_lengths,
    first_pos,
):
    logits = jnp.einsum(
        "zxm,zum->zxu",
        compressed_absorbed_queries,
        compressed_stored_keys,
        preferred_element_type=jnp.float32,
    )
    logits = logits + jnp.einsum(
        "srh,srl->shl", query_rope, cache_rope, preferred_element_type=jnp.float32
    )
    logits = logits * (NOPE + query_rope.shape[1]) ** (-0.5)
    position = first_pos + jnp.arange(compressed_stored_keys.shape[1], dtype=jnp.int32)
    visible = position[None, None, :] < seq_lengths[:, None, None]
    logits = jnp.where(visible, logits, NEGATIVE_PADDING)
    top_score = jnp.max(logits, axis=2)
    weights = jnp.where(visible, jnp.exp(logits - top_score[:, :, None]), 0.0)
    denominator = jnp.sum(weights, axis=2)
    weighted = jnp.einsum(
        "jac,jcw->jaw",
        weights.astype(jnp.bfloat16),
        compressed_stored_keys,
        preferred_element_type=jnp.float32,
    )
    return top_score, denominator, weighted


def packed_attention(queries, query_rope, keys, cache_rope, seq_lengths, column):
    cols = lax.axis_size(COL)
    seqs, heads, _ = queries.shape
    top_score, denominator, weighted = local_partials(
        queries, query_rope, keys, cache_rope, seq_lengths, column * keys.shape[1]
    )
    packed = with_columns(weighted, halves_of(top_score, 3) + halves_of(denominator, 3))
    return jnp.moveaxis(packed.reshape(seqs, cols, heads // cols, -1), 1, 0)


def merged_attention(packed, latent):
    merged = exchanged(row_major(packed))
    merged = merged.astype(jnp.float32)
    tops = merged[..., latent] + (merged[..., latent + 1] + merged[..., latent + 2])
    totals = merged[..., latent + 3] + (merged[..., latent + 4] + merged[..., latent + 5])
    factor = jnp.exp(tops - jnp.max(tops, axis=0, keepdims=True))
    total = jnp.sum(totals * factor, axis=0)
    context = jnp.sum(merged[..., :latent] * factor[..., None], axis=0)
    return (context / total[..., None]).astype(jnp.bfloat16)


def summed_near(partial):
    far, size = partial.shape[:2]
    near = lax.axis_index(NEAR)
    window = size // 2
    place, side = near % window, near // window
    partial = partial.reshape(2 * far, window, *partial.shape[2:])

    def block(blocks, k):
        return lax.dynamic_index_in_dim(blocks, k, 1, keepdims=False)

    half = window // 2
    sends = [((place + half) % window, half, -half)]
    for hops in range(half - 1, 0, -1):
        sends += [((place + hops) % window, hops, hops)]
        sends += [((place + window - hops) % window, -hops, -hops)]
    blocks = [block(partial, send[0]) for send in sends]
    arrived = [along_lane(b, *send[1:]) for b, send in zip(blocks, sends)]
    total = block(partial, place).astype(jnp.float32)
    for other in arrived:
        total = total + other.astype(jnp.float32)
    total = total.astype(jnp.bfloat16).reshape(far, 2, *partial.shape[2:])
    sent = block(total, 1 - side)
    other = along_lane(sent, window, -window)
    total = block(total, side).astype(jnp.float32) + other.astype(jnp.float32)
    return total.astype(jnp.bfloat16)


def stage_kernel(gate_ref, up_ref, gain_ref, both_ref, gain_out_ref, arrived):
    units = gate_ref.shape[0]
    copies = [
        pltpu.make_async_copy(gate_ref, both_ref.at[pl.ds(0, units)], arrived.at[0]),
        pltpu.make_async_copy(up_ref, both_ref.at[pl.ds(units, units)], arrived.at[1]),
        pltpu.make_async_copy(gain_ref, gain_out_ref, arrived.at[2]),
    ]
    for copy in copies:
        copy.start()
    for copy in copies:
        copy.wait()


def staged(gate, up, gain):
    units, width = gate.shape
    anywhere = pl.BlockSpec(memory_space=pl.ANY)
    return pl.pallas_call(
        stage_kernel,
        out_shape=(
            jax.ShapeDtypeStruct((2 * units, width), gate.dtype),
            jax.ShapeDtypeStruct(gain.shape, gain.dtype),
        ),
        in_specs=[anywhere] * 3,
        out_specs=(anywhere, anywhere),
        scratch_shapes=[pltpu.SemaphoreType.DMA((3,))],
        compiler_params=pltpu.CompilerParams(vmem_limit_bytes=1 << 20),
        name="staged",
    )(gate, up, gain)


def project_kernel(x_ref, gain_ref, *refs):
    *w_refs, out_ref, w_vmem, arrived = refs
    rows = w_refs[0].shape[0]
    copies = [
        pltpu.make_async_copy(w_ref, w_vmem.at[pl.ds(k * rows, rows)], arrived.at[k])
        for k, w_ref in enumerate(w_refs)
    ]
    for copy in copies:
        copy.start()
    cols, _, tokens = out_ref.shape
    projections = 2 * len(copies)
    units = rows // 2
    share = units // cols
    x = x_ref[...].astype(jnp.float32)
    scaled = (x * gain_ref[...].astype(jnp.float32)).astype(jnp.bfloat16)
    squares = jnp.sum(x * x, axis=1, keepdims=True)
    squares = jnp.broadcast_to(squares, (tokens, 128)).T[:8]
    coarse = squares.astype(jnp.bfloat16).astype(jnp.float32)
    row = lax.broadcasted_iota(jnp.int32, squares.shape, 0)
    norms = jnp.where(row == 0, coarse, squares - coarse).astype(jnp.bfloat16)
    for c in range(cols):
        out_ref[c, projections * share :, :] = norms
    for copy in copies:
        copy.wait()
    product = lax.dot_general(
        w_vmem[...], scaled, (((1,), (1,)), ((), ())), preferred_element_type=jnp.float32
    ).astype(jnp.bfloat16)
    for k in range(projections):
        for c in range(cols):
            start = k * units + c * share
            out_ref[c, k * share : (k + 1) * share, :] = product[start : start + share, :]


def projected(gathered, gain, weights, cols):
    tokens, width = gathered.shape
    units = len(weights) * weights[0].shape[0]
    whole = pl.BlockSpec(memory_space=pltpu.VMEM)
    return pl.pallas_call(
        project_kernel,
        out_shape=jax.ShapeDtypeStruct((cols, units // cols + 8, tokens), jnp.bfloat16),
        in_specs=[whole, whole] + [pl.BlockSpec(memory_space=pl.ANY)] * len(weights),
        out_specs=whole,
        scratch_shapes=[
            pltpu.VMEM((units, width), jnp.bfloat16),
            pltpu.SemaphoreType.DMA((len(weights),)),
        ],
        compiler_params=pltpu.CompilerParams(vmem_limit_bytes=24 << 20),
        cost_estimate=pl.CostEstimate(
            flops=2 * units * width * tokens,
            bytes_accessed=2 * units * width,
            transcendentals=0,
        ),
        name="projected",
    )(gathered, gain, *weights)


def feed_forward(ffn_rows, norm_gain, w_gate, w_up, w_down, queries):
    cols = lax.axis_size(COL)
    rows, width = ffn_rows.shape
    units = w_gate.shape[1]
    share = units // cols
    into, gain = staged(w_gate.T, w_up.T, norm_gain)
    into = [into, swapped(into)]
    gathered = gathered_on_lane(ffn_rows)

    packed = projected(gathered, gain, into, cols)
    packed, w_down, *queries = lax.optimization_barrier((packed, w_down, *queries))
    out_of = [w_down, swapped(w_down)]
    total = exchanged(packed)
    total = jnp.sum(total.astype(jnp.float32), axis=0)
    mean_square = (total[4 * share] + total[4 * share + 1]) / (width * cols)
    scale = lax.rsqrt(mean_square + 1e-06)[None, :]
    total = (total[: 4 * share] * scale).reshape(2, 2, share, -1)
    hidden = (jax.nn.silu(total[:, 0]) * total[:, 1]).astype(jnp.bfloat16)

    hidden = row_major(jnp.broadcast_to(hidden, (cols, *hidden.shape)))
    hidden = exchanged(hidden)
    partial = sum(
        lax.dot_general(
            hidden[:, k].reshape(units, -1),
            w,
            (((0,), (0,)), ((), ())),
            preferred_element_type=jnp.float32,
        )
        for k, w in enumerate(out_of)
    )
    partial = partial.astype(jnp.bfloat16)
    partial = partial.reshape(lax.axis_size(FAR), lax.axis_size(NEAR), rows, width)
    return partial, queries


def on_device(
    compressed_absorbed_queries,
    query_rope,
    compressed_stored_keys,
    cache_rope,
    seq_lengths,
    ffn_rows,
    norm_gain,
    w_gate,
    w_up,
    w_down,
):
    column = lax.axis_index(COL)
    partial, queries = feed_forward(
        ffn_rows,
        norm_gain,
        w_gate,
        w_up,
        w_down,
        (compressed_absorbed_queries, query_rope, cache_rope, seq_lengths, column),
    )
    queries, query_rope, cache_rope, seq_lengths, position = queries
    packed = packed_attention(
        queries, query_rope, compressed_stored_keys, cache_rope, seq_lengths, position
    )
    near = summed_near(partial)
    pieces = lax.all_to_all(row_major(near), FAR, 0, 0, tiled=True)
    reduced = jnp.sum(pieces.astype(jnp.float32), axis=0)
    context = merged_attention(packed, compressed_stored_keys.shape[-1])
    ffn_out = (ffn_rows.astype(jnp.float32) + reduced).astype(jnp.bfloat16)
    return (context, ffn_out)


def solution(mesh):
    chips = mesh.shape["row"] // 2
    finer = Mesh(
        mesh.devices.reshape(
            mesh.shape["group"], chips // NEAR_CHIPS, NEAR_CHIPS, 2, mesh.shape["col"]
        ),
        ("group", *ROW, COL),
    )
    return jax.shard_map(
        on_device,
        mesh=finer,
        in_specs=(
            P(GROUP_ROW, None, None),
            P(GROUP_ROW, None, None),
            P(GROUP_ROW, COL, None),
            P(GROUP_ROW, None, COL),
            P(GROUP_ROW),
            P(GROUP_ROW, COL),
            P(COL),
            P(COL, ROW),
            P(COL, ROW),
            P(ROW, COL),
        ),
        out_specs=(P(GROUP_ROW, COL, None), P(GROUP_ROW, COL)),
        check_vma=False,
    )
```

```python
import jax
import jax.numpy as jnp
from jax import lax
from jax.experimental import pallas as pl
from jax.experimental.pallas import tpu as pltpu
from jax.experimental.layout import Layout, with_layout_constraint
from jax.sharding import Mesh
from jax.sharding import PartitionSpec as P


NOPE = 128
FAR, NEAR, CORE, COL = "row_far", "row_near", "row_core", "col"
CHIP = (FAR, NEAR)
ROW = (FAR, NEAR, CORE)
GROUP_ROW = ("group", *ROW)
NEAR_CHIPS = 8

NEGATIVE_PADDING = -1e30


def row_major(x):
    return with_layout_constraint(x, Layout(major_to_minor=tuple(range(x.ndim))))


def on_lane(chip, lane):
    return 2 * chip + (lane + chip) % 2


def along_lane(x, hops_of_first, hops_of_second):
    chips = lax.axis_size(CHIP)
    pairs = [
        (on_lane(z, lane), on_lane((z + hops) % chips, lane))
        for lane, hops in enumerate((hops_of_first, hops_of_second))
        for z in range(chips)
    ]
    return lax.ppermute(x, ROW, pairs)


def gathered_on_lane(x):
    chips = lax.axis_size(CHIP)
    lanes = [[on_lane(z, lane) for z in range(chips)] for lane in (0, 1)]
    return lax.all_gather(x, ROW, axis_index_groups=lanes, axis=0, tiled=True)


def swapped(x):
    return lax.ppermute(x, CORE, [(0, 1), (1, 0)])


def exchanged(pieces):
    return lax.all_to_all(pieces, COL, split_axis=0, concat_axis=0, tiled=True)


def halves_of(x, count):
    pieces = []
    for _ in range(count - 1):
        coarse = lax.reduce_precision(x, 8, 7)
        pieces.append(coarse)
        x = x - coarse
    return pieces + [x]


def with_columns(x, columns):
    extra = jnp.stack(columns, axis=-1).astype(jnp.bfloat16)
    extra = jnp.pad(extra, [(0, 0)] * (x.ndim - 1) + [(0, 128 - len(columns))])
    return jnp.concatenate([x.astype(jnp.bfloat16), extra], axis=-1)


def local_partials(
    compressed_absorbed_queries,
    query_rope,
    compressed_stored_keys,
    cache_rope,
    seq_lengths,
    first_pos,
):
    logits = jnp.einsum(
        "zxm,zum->zxu",
        compressed_absorbed_queries,
        compressed_stored_keys,
        preferred_element_type=jnp.float32,
    )
    logits = logits + jnp.einsum(
        "srh,srl->shl", query_rope, cache_rope, preferred_element_type=jnp.float32
    )
    logits = logits * (NOPE + query_rope.shape[1]) ** (-0.5)
    position = first_pos + jnp.arange(compressed_stored_keys.shape[1], dtype=jnp.int32)
    visible = position[None, None, :] < seq_lengths[:, None, None]
    logits = jnp.where(visible, logits, NEGATIVE_PADDING)
    top_score = jnp.max(logits, axis=2)
    weights = jnp.where(visible, jnp.exp(logits - top_score[:, :, None]), 0.0)
    denominator = jnp.sum(weights, axis=2)
    weighted = jnp.einsum(
        "jac,jcw->jaw",
        weights.astype(jnp.bfloat16),
        compressed_stored_keys,
        preferred_element_type=jnp.float32,
    )
    return top_score, denominator, weighted


def packed_attention(queries, query_rope, keys, cache_rope, seq_lengths, column):
    cols = lax.axis_size(COL)
    seqs, heads, _ = queries.shape
    top_score, denominator, weighted = local_partials(
        queries, query_rope, keys, cache_rope, seq_lengths, column * keys.shape[1]
    )
    packed = with_columns(weighted, halves_of(top_score, 3) + halves_of(denominator, 3))
    return jnp.moveaxis(packed.reshape(seqs, cols, heads // cols, -1), 1, 0)


def merged_attention(packed, latent):
    merged = exchanged(row_major(packed))
    merged = merged.astype(jnp.float32)
    tops = merged[..., latent] + (merged[..., latent + 1] + merged[..., latent + 2])
    totals = merged[..., latent + 3] + (merged[..., latent + 4] + merged[..., latent + 5])
    factor = jnp.exp(tops - jnp.max(tops, axis=0, keepdims=True))
    total = jnp.sum(totals * factor, axis=0)
    context = jnp.sum(merged[..., :latent] * factor[..., None], axis=0)
    return (context / total[..., None]).astype(jnp.bfloat16)


def summed_near(partial):
    far, size = partial.shape[:2]
    near = lax.axis_index(NEAR)
    window = size // 2
    place, side = near % window, near // window
    partial = partial.reshape(2 * far, window, *partial.shape[2:])

    def block(blocks, k):
        return lax.dynamic_index_in_dim(blocks, k, 1, keepdims=False)

    half = window // 2
    sends = [((place + half) % window, half, -half)]
    for hops in range(half - 1, 0, -1):
        sends += [((place + hops) % window, hops, hops)]
        sends += [((place + window - hops) % window, -hops, -hops)]
    blocks = [block(partial, send[0]) for send in sends]
    arrived = [along_lane(b, *send[1:]) for b, send in zip(blocks, sends)]
    total = block(partial, place).astype(jnp.float32)
    for other in arrived:
        total = total + other.astype(jnp.float32)
    total = total.astype(jnp.bfloat16).reshape(far, 2, *partial.shape[2:])
    sent = block(total, 1 - side)
    other = along_lane(sent, window, -window)
    total = block(total, side).astype(jnp.float32) + other.astype(jnp.float32)
    return total.astype(jnp.bfloat16)


def stage_kernel(gate_ref, up_ref, gain_ref, both_ref, gain_out_ref, arrived):
    units = gate_ref.shape[0]
    copies = [
        pltpu.make_async_copy(gate_ref, both_ref.at[pl.ds(0, units)], arrived.at[0]),
        pltpu.make_async_copy(up_ref, both_ref.at[pl.ds(units, units)], arrived.at[1]),
        pltpu.make_async_copy(gain_ref, gain_out_ref, arrived.at[2]),
    ]
    for copy in copies:
        copy.start()
    for copy in copies:
        copy.wait()


def staged(gate, up, gain):
    units, width = gate.shape
    anywhere = pl.BlockSpec(memory_space=pl.ANY)
    return pl.pallas_call(
        stage_kernel,
        out_shape=(
            jax.ShapeDtypeStruct((2 * units, width), gate.dtype),
            jax.ShapeDtypeStruct(gain.shape, gain.dtype),
        ),
        in_specs=[anywhere] * 3,
        out_specs=(anywhere, anywhere),
        scratch_shapes=[pltpu.SemaphoreType.DMA((3,))],
        compiler_params=pltpu.CompilerParams(vmem_limit_bytes=1 << 20),
        name="staged",
    )(gate, up, gain)


def project_kernel(x_ref, gain_ref, own_ref, other_ref, out_ref, other_vmem, arrived):
    copy = pltpu.make_async_copy(other_ref, other_vmem, arrived)
    copy.start()
    cols, _, tokens = out_ref.shape
    units = own_ref.shape[0] // 2
    share = units // cols
    x = x_ref[...].astype(jnp.float32)
    scaled = (x * gain_ref[...].astype(jnp.float32)).astype(jnp.bfloat16)
    squares = jnp.sum(x * x, axis=1, keepdims=True)
    squares = jnp.broadcast_to(squares, (tokens, 128)).T[:8]
    coarse = squares.astype(jnp.bfloat16).astype(jnp.float32)
    row = lax.broadcasted_iota(jnp.int32, squares.shape, 0)
    norms = jnp.where(row == 0, coarse, squares - coarse).astype(jnp.bfloat16)
    for c in range(cols):
        out_ref[c, 4 * share :, :] = norms

    def write(weights, first):
        product = lax.dot_general(
            weights, scaled, (((1,), (1,)), ((), ())), preferred_element_type=jnp.float32
        ).astype(jnp.bfloat16)
        for k in range(2):
            for c in range(cols):
                start = k * units + c * share
                to = (first + k) * share
                out_ref[c, to : to + share, :] = product[start : start + share, :]

    write(own_ref[...], 0)
    copy.wait()
    write(other_vmem[...], 2)


def projected(gathered, gain, own, other, cols):
    tokens, width = gathered.shape
    units = own.shape[0] + other.shape[0]
    whole = pl.BlockSpec(memory_space=pltpu.VMEM)
    return pl.pallas_call(
        project_kernel,
        out_shape=jax.ShapeDtypeStruct((cols, units // cols + 8, tokens), jnp.bfloat16),
        in_specs=[whole, whole, whole, pl.BlockSpec(memory_space=pl.ANY)],
        out_specs=whole,
        scratch_shapes=[pltpu.VMEM(other.shape, other.dtype), pltpu.SemaphoreType.DMA],
        compiler_params=pltpu.CompilerParams(vmem_limit_bytes=24 << 20),
        cost_estimate=pl.CostEstimate(
            flops=2 * units * width * tokens,
            bytes_accessed=2 * units * width,
            transcendentals=0,
        ),
        name="projected",
    )(gathered, gain, own, other)


def feed_forward(ffn_rows, norm_gain, w_gate, w_up, w_down, queries):
    cols = lax.axis_size(COL)
    rows, width = ffn_rows.shape
    units = w_gate.shape[1]
    share = units // cols
    into, gain = staged(w_gate.T, w_up.T, norm_gain)
    partners = swapped(into)
    gathered = gathered_on_lane(ffn_rows)

    packed = projected(gathered, gain, into, partners, cols)
    packed, w_down, *queries = lax.optimization_barrier((packed, w_down, *queries))
    out_of = [w_down, swapped(w_down)]
    total = exchanged(packed)
    total = jnp.sum(total.astype(jnp.float32), axis=0)
    mean_square = (total[4 * share] + total[4 * share + 1]) / (width * cols)
    scale = lax.rsqrt(mean_square + 1e-06)[None, :]
    total = (total[: 4 * share] * scale).reshape(2, 2, share, -1)
    hidden = (jax.nn.silu(total[:, 0]) * total[:, 1]).astype(jnp.bfloat16)

    hidden = row_major(jnp.broadcast_to(hidden, (cols, *hidden.shape)))
    hidden = exchanged(hidden)
    partial = sum(
        lax.dot_general(
            hidden[:, k].reshape(units, -1),
            w,
            (((0,), (0,)), ((), ())),
            preferred_element_type=jnp.float32,
        )
        for k, w in enumerate(out_of)
    )
    partial = partial.astype(jnp.bfloat16)
    partial = partial.reshape(lax.axis_size(FAR), lax.axis_size(NEAR), rows, width)
    return partial, queries


def on_device(
    compressed_absorbed_queries,
    query_rope,
    compressed_stored_keys,
    cache_rope,
    seq_lengths,
    ffn_rows,
    norm_gain,
    w_gate,
    w_up,
    w_down,
):
    column = lax.axis_index(COL)
    partial, queries = feed_forward(
        ffn_rows,
        norm_gain,
        w_gate,
        w_up,
        w_down,
        (compressed_absorbed_queries, query_rope, cache_rope, seq_lengths, column),
    )
    queries, query_rope, cache_rope, seq_lengths, position = queries
    packed = packed_attention(
        queries, query_rope, compressed_stored_keys, cache_rope, seq_lengths, position
    )
    near = summed_near(partial)
    pieces = lax.all_to_all(row_major(near), FAR, 0, 0, tiled=True)
    reduced = jnp.sum(pieces.astype(jnp.float32), axis=0)
    context = merged_attention(packed, compressed_stored_keys.shape[-1])
    ffn_out = (ffn_rows.astype(jnp.float32) + reduced).astype(jnp.bfloat16)
    return (context, ffn_out)


def solution(mesh):
    chips = mesh.shape["row"] // 2
    finer = Mesh(
        mesh.devices.reshape(
            mesh.shape["group"], chips // NEAR_CHIPS, NEAR_CHIPS, 2, mesh.shape["col"]
        ),
        ("group", *ROW, COL),
    )
    return jax.shard_map(
        on_device,
        mesh=finer,
        in_specs=(
            P(GROUP_ROW, None, None),
            P(GROUP_ROW, None, None),
            P(GROUP_ROW, COL, None),
            P(GROUP_ROW, None, COL),
            P(GROUP_ROW),
            P(GROUP_ROW, COL),
            P(COL),
            P(COL, ROW),
            P(COL, ROW),
            P(ROW, COL),
        ),
        out_specs=(P(GROUP_ROW, COL, None), P(GROUP_ROW, COL)),
        check_vma=False,
    )
```
